16 devices in a mesh: tp: 2 (over z), dp: 8 (over y, x, core).
Axes of the slice: x: 2, y: 2, z: 2, core: 2. Of those that a mesh axis runs over, the one named last changes fastest.
Arguments:
- token_ids: int32 [256, 256], P('dp')
- embed_table: bfloat16 [50304, 1024], P('tp')
- ln1_gain: bfloat16 [1024], replicated
- ln1_bias: bfloat16 [1024], replicated
- ln2_gain: bfloat16 [1024], replicated
- ln2_bias: bfloat16 [1024], replicated
- w_qkv: bfloat16 [1024, 16, 3, 64], P(None, 'tp')
- b_qkv: bfloat16 [16, 3, 64], P('tp')
- w_dense: bfloat16 [16, 64, 1024], P('tp')
- b_dense: bfloat16 [1024], replicated
- w_fc1: bfloat16 [1024, 4096], P(None, 'tp')
- b_fc1: bfloat16 [4096], P('tp')
- w_fc2: bfloat16 [4096, 1024], P('tp')
- b_fc2: bfloat16 [1024], replicated
- cotangent: bfloat16 [256, 256, 1024], P('dp')
Outputs:
- output 1: bfloat16 [256, 256, 1024], P('dp')
- output 2: float32 [50304, 1024], P('tp', 'dp')
- output 3: float32 [1024], P('dp')
- output 4: float32 [1024], P('dp')
- output 5: float32 [1024], P('dp')
- output 6: float32 [1024], P('dp')
- output 7: float32 [1024, 16, 3, 64], P('dp', 'tp')
- output 8: float32 [3072], P(('tp', 'dp'))
- output 9: float32 [16, 64, 1024], P('tp', None, 'dp')
- output 10: float32 [1024], P('dp')
- output 11: float32 [1024, 4096], P('dp', 'tp')
- output 12: float32 [4096], P(('tp', 'dp'))
- output 13: float32 [4096, 1024], P('tp', 'dp')
- output 14: float32 [1024], P('dp')
All inputs are finite; a program needn't handle non-finite values.
Results may differ from the reference program's by a relative error of at most 0.0100979.
Values sent between devices are 32-bit elements.
A program may use at most 1 GiB of HBM per device.

```python
import jax
import jax.numpy as jnp
from jax import lax

VOCAB_SIZE = 50304
D_MODEL = 1024
N_HEADS = 16
HEAD_DIM = 64
FF_DIM = 4096
SEQ_LEN = 256
BATCH_SEQS = 256
ROT_DIM = HEAD_DIM // 4
EPS_NORM = 1e-5
ROPE_BASE = 10000.0


def setup_inputs(seed: int = 0) -> dict:
    key_list = jax.random.split(jax.random.key(seed), 16)
    base_ids = jax.random.randint(key_list[0], (BATCH_SEQS, SEQ_LEN), 0, VOCAB_SIZE, dtype=jnp.int32)
    shifts = jax.random.randint(key_list[1], (BATCH_SEQS, SEQ_LEN), 0, 8, dtype=jnp.int32)
    token_ids = jnp.right_shift(base_ids, shifts)
    token_ids = token_ids.at[0, 0].set(VOCAB_SIZE - 1).at[0, 1].set(0)
    d_scale = D_MODEL ** -0.5
    f_scale = FF_DIM ** -0.5

    def draw_normal(key_index, arr_shape, spread, offset):
        sample = jax.random.normal(key_list[key_index], arr_shape, jnp.float32) * spread + offset
        return sample.astype(jnp.bfloat16)

    return {
        'token_ids': token_ids,
        'embed_table': draw_normal(2, (VOCAB_SIZE, D_MODEL), 1.0, 0.0),
        'ln1_gain': draw_normal(3, (D_MODEL,), 0.6, 1.0),
        'ln1_bias': draw_normal(4, (D_MODEL,), 0.5, 0.0),
        'ln2_gain': draw_normal(5, (D_MODEL,), 0.6, 1.0),
        'ln2_bias': draw_normal(6, (D_MODEL,), 0.5, 0.0),
        'w_qkv': draw_normal(7, (D_MODEL, N_HEADS, 3, HEAD_DIM), d_scale, 0.0),
        'b_qkv': draw_normal(8, (N_HEADS, 3, HEAD_DIM), 0.5, 0.0),
        'w_dense': draw_normal(9, (N_HEADS, HEAD_DIM, D_MODEL), d_scale, 0.0),
        'b_dense': draw_normal(10, (D_MODEL,), 1.0, 0.0),
        'w_fc1': draw_normal(11, (D_MODEL, FF_DIM), d_scale, 0.0),
        'b_fc1': draw_normal(12, (FF_DIM,), 0.5, 0.0),
        'w_fc2': draw_normal(13, (FF_DIM, D_MODEL), f_scale, 0.0),
        'b_fc2': draw_normal(14, (D_MODEL,), 1.0, 0.0),
        'cotangent': draw_normal(15, (BATCH_SEQS, SEQ_LEN, D_MODEL), 1.0, 0.0),
    }


def to_bf16(tensor):
    return tensor.astype(jnp.bfloat16).astype(jnp.float32)


def rope_tables():
    half_rot = ROT_DIM // 2
    inv_freq = ROPE_BASE ** (-(jnp.arange(half_rot, dtype=jnp.float32) * 2.0) / ROT_DIM)
    angles = jnp.arange(SEQ_LEN, dtype=jnp.float32)[:, None] * inv_freq[None, :]
    angles = jnp.concatenate([angles, angles], axis=-1)
    return jnp.cos(angles)[:, None, :], jnp.sin(angles)[:, None, :]


def apply_rope(tensor, cos_table, sin_table):
    half_rot = ROT_DIM // 2
    rot_part = tensor[..., :ROT_DIM]
    turned = jnp.concatenate([-rot_part[..., half_rot:], rot_part[..., :half_rot]], axis=-1)
    return jnp.concatenate([rot_part * cos_table + turned * sin_table, tensor[..., ROT_DIM:]], axis=-1)


def layer_seq(x_seq, params):
    (ln1_gain, ln1_bias, ln2_gain, ln2_bias, w_qkv, b_qkv, w_dense, b_dense, w_fc1, b_fc1, w_fc2, b_fc2) = params
    mean_x = jnp.mean(x_seq, axis=-1, keepdims=True)
    centered = x_seq - mean_x
    normed = centered * lax.rsqrt(jnp.mean(centered * centered, axis=-1, keepdims=True) + EPS_NORM)
    hid_attn = to_bf16(normed * ln1_gain + ln1_bias)
    hid_mlp = to_bf16(normed * ln2_gain + ln2_bias)
    qkv_all = to_bf16(jnp.einsum('sd,dhjc->shjc', hid_attn, w_qkv) + b_qkv)
    cos_table, sin_table = rope_tables()
    queries = to_bf16(apply_rope(qkv_all[:, :, 0], cos_table, sin_table))
    keys_rot = to_bf16(apply_rope(qkv_all[:, :, 1], cos_table, sin_table))
    values = qkv_all[:, :, 2]
    scores = jnp.einsum('qhc,khc->hqk', queries, keys_rot) * HEAD_DIM ** -0.5
    causal = jnp.arange(SEQ_LEN)[:, None] >= jnp.arange(SEQ_LEN)[None, :]
    probs_low = to_bf16(jax.nn.softmax(jnp.where(causal[None], scores, -1e30), axis=-1))
    context = to_bf16(jnp.einsum('hqk,khc->qhc', probs_low, values))
    attn_out = jnp.einsum('qhc,hcd->qd', context, w_dense) + b_dense
    pre_act = to_bf16(jnp.dot(hid_mlp, w_fc1, preferred_element_type=jnp.float32) + b_fc1)
    gelu_out = to_bf16(jax.nn.gelu(pre_act, approximate=False))
    mlp_out = jnp.dot(gelu_out, w_fc2, preferred_element_type=jnp.float32) + b_fc2
    return to_bf16(x_seq + attn_out + mlp_out)


def reference(token_ids, embed_table, ln1_gain, ln1_bias, ln2_gain, ln2_bias, w_qkv, b_qkv, w_dense, b_dense, w_fc1, b_fc1, w_fc2, b_fc2, cotangent):
    params = tuple(item.astype(jnp.float32) for item in (ln1_gain, ln1_bias, ln2_gain, ln2_bias, w_qkv, b_qkv, w_dense, b_dense, w_fc1, b_fc1, w_fc2, b_fc2))
    tokens = jnp.take(embed_table, token_ids, axis=0)
    zero_grads = tuple(jnp.zeros_like(item) for item in params)
    zero_embed = jnp.zeros((VOCAB_SIZE, D_MODEL), jnp.float32)

    def scan_step(carry, inputs):
        grad_acc, embed_acc = carry
        tok_seq, ids_seq, cot_seq = inputs
        out_seq, vjp_pull = jax.vjp(layer_seq, tok_seq.astype(jnp.float32), params)
        grad_x, grad_params = vjp_pull(cot_seq.astype(jnp.float32))
        grad_acc = tuple(acc_item + new_item for acc_item, new_item in zip(grad_acc, grad_params))
        embed_acc = embed_acc.at[ids_seq].add(grad_x)
        return (grad_acc, embed_acc), out_seq.astype(jnp.bfloat16)

    (grads, d_embed), layer_out = lax.scan(scan_step, (zero_grads, zero_embed), (tokens, token_ids, cotangent))
    (d_ln1_gain, d_ln1_bias, d_ln2_gain, d_ln2_bias, d_w_qkv, d_b_qkv, d_w_dense, d_b_dense, d_w_fc1, d_b_fc1, d_w_fc2, d_b_fc2) = grads
    return (layer_out, d_embed, d_ln1_gain, d_ln1_bias, d_ln2_gain, d_ln2_bias, d_w_qkv, d_b_qkv.reshape(-1), d_w_dense, d_b_dense, d_w_fc1, d_b_fc1, d_w_fc2, d_b_fc2)
```

```python
import functools
import jax
import jax.numpy as jnp
from jax import lax
from jax.experimental import pallas as pl
from jax.experimental.pallas import tpu as pltpu
from jax.sharding import PartitionSpec as P

EPS_NORM = 1e-5
ROPE_BASE = 10000.0
CHUNKS = (4, 6, 6)
HALF_ROOT = 0.5 ** 0.5
PDF_SCALE = (2.0 * 3.141592653589793) ** -0.5
F32, BF16 = jnp.float32, jnp.bfloat16


def dot_f32(a, b, dims):
    return lax.dot_general(a, b, (dims, ((), ())), preferred_element_type=F32)


def rope_consts(seq_len, head_dim):
    rot_dim = head_dim // 4
    half_rot = rot_dim // 2
    inv_freq = ROPE_BASE ** (-(jnp.arange(half_rot, dtype=F32) * 2.0) / rot_dim)
    angles = jnp.arange(seq_len, dtype=F32)[:, None] * inv_freq[None, :]
    angles = jnp.concatenate([angles, angles], axis=-1)
    rest = (seq_len, head_dim - rot_dim)
    cos_head = jnp.concatenate([jnp.cos(angles), jnp.ones(rest, F32)], axis=-1)
    sin_head = jnp.concatenate([jnp.sin(angles), jnp.zeros(rest, F32)], axis=-1)
    row = jnp.arange(2 * head_dim)[:, None]
    col = jnp.arange(2 * head_dim)[None, :]
    ch = col % head_dim
    turn = jnp.where((ch < half_rot) & (row == col + half_rot), -1.0, 0.0) + jnp.where((ch >= half_rot) & (ch < rot_dim) & (row == col - half_rot), 1.0, 0.0)
    return jnp.tile(cos_head, (1, 2)), jnp.tile(sin_head, (1, 2)), turn.astype(BF16)


def attention_kernel(head_dim, q_ref, k_ref, v_ref, g_ref, cos_ref, sin_ref, turn_ref, ctx_ref, dq_ref, dk_ref, dv_ref):
    seq_len, width = q_ref.shape[1], q_ref.shape[2]
    pair = 2 * head_dim
    scale = head_dim ** -0.5
    cos, sin, turn = cos_ref[...], sin_ref[...], turn_ref[...]
    low = lax.broadcasted_iota(jnp.int32, (seq_len, pair), 1) < head_dim
    causal = lax.broadcasted_iota(jnp.int32, (seq_len, seq_len), 0) >= lax.broadcasted_iota(jnp.int32, (seq_len, seq_len), 1)

    def rotate(val):
        turned = dot_f32(val, turn, ((1,), (0,)))
        return (val.astype(F32) * cos + turned * sin).astype(BF16)

    def unrotate(grad):
        turned = dot_f32(grad, turn, ((1,), (1,)))
        return (grad.astype(F32) * cos + turned * sin).astype(BF16)

    def step(j, carry):
        cols = pl.ds(pl.multiple_of(j * pair, pair), pair)
        q = rotate(q_ref[0, :, cols])
        k = rotate(k_ref[0, :, cols])
        v = v_ref[0, :, cols]
        g = g_ref[0, :, cols]
        parts = []
        for head in range(2):
            mine = low if head == 0 else jnp.logical_not(low)
            q_h = jnp.where(mine, q, jnp.zeros_like(q))
            g_h = jnp.where(mine, g, jnp.zeros_like(g))
            scores = dot_f32(q_h, k, ((1,), (1,))) * scale
            scores = jnp.where(causal, scores, -1e30)
            top = jnp.max(scores, axis=-1, keepdims=True)
            expo = jnp.exp(scores - top)
            soft = expo * (1.0 / jnp.sum(expo, axis=-1, keepdims=True))
            probs = soft.astype(BF16)
            ctx = dot_f32(probs, v, ((1,), (0,)))
            d_probs = dot_f32(g_h, v, ((1,), (1,))).astype(BF16).astype(F32)
            d_v = dot_f32(probs, g, ((0,), (0,)))
            inner = jnp.sum(soft * d_probs, axis=-1, keepdims=True)
            d_s = (soft * (d_probs - inner) * scale).astype(BF16)
            d_q = dot_f32(d_s, k, ((1,), (0,)))
            d_k = dot_f32(d_s, q, ((0,), (0,)))
            parts.append((ctx, d_q, d_k, d_v))
        ctx, d_q, d_k, d_v = (jnp.where(low, a, b).astype(BF16) for a, b in zip(*parts))
        ctx_ref[0, :, cols] = ctx
        dq_ref[0, :, cols] = unrotate(d_q)
        dk_ref[0, :, cols] = unrotate(d_k)
        dv_ref[0, :, cols] = d_v
        return carry

    lax.fori_loop(0, width // pair, step, 0)


def attention(q, k, v, g, consts, head_dim):
    n, seq_len, width = q.shape
    big = pl.BlockSpec((1, seq_len, width), lambda i: (i, 0, 0))
    const = [pl.BlockSpec(c.shape, lambda i: (0, 0)) for c in consts]
    shape = jax.ShapeDtypeStruct(q.shape, BF16)
    flops = n * (width // head_dim) * 12 * seq_len * seq_len * 2 * head_dim
    return pl.pallas_call(
        functools.partial(attention_kernel, head_dim),
        grid=(n,),
        in_specs=[big] * 4 + const,
        out_specs=[big] * 4,
        out_shape=[shape] * 4,
        compiler_params=pltpu.CompilerParams(dimension_semantics=("arbitrary",), vmem_limit_bytes=40 * 1024 * 1024),
        cost_estimate=pl.CostEstimate(flops=4 * flops, bytes_accessed=16 * q.size, transcendentals=0),
        name="attention",
    )(q, k, v, g, *consts)


def scatter_kernel(has_init, rows, block, counts, *refs):
    n_arr = len(counts)
    ids_refs, g_refs, rest = refs[:n_arr], refs[n_arr:2 * n_arr], refs[2 * n_arr:]
    if has_init:
        init_ref, out_ref, acc0, acc1, sem = rest
    else:
        out_ref, acc0, acc1, sem = rest
    step = pl.program_id(0)
    padded = acc0.shape[0]
    group = 32

    @pl.when(step == 0)
    def _():
        def clear(i, carry):
            at = pl.ds(pl.multiple_of(i * 8, 8), 8)
            acc1[at, :] = jnp.zeros((8, acc1.shape[1]), F32)
            if not has_init:
                acc0[at, :] = jnp.zeros((8, acc0.shape[1]), F32)
            return carry
        lax.fori_loop(0, padded // 8, clear, 0, unroll=8)
        if has_init:
            copy = pltpu.make_async_copy(init_ref, acc0.at[pl.ds(0, rows)], sem)
            copy.start()
            copy.wait()

    first = 0
    for ids_ref, g_ref, count in zip(ids_refs, g_refs, counts):
        def add_block(ids_ref=ids_ref, g_ref=g_ref):
            def add_group(i, carry):
                for u in range(0, group, 2):
                    at = i * group + u
                    r0 = ids_ref[0, 0, at]
                    r1 = ids_ref[0, 0, at + 1]
                    acc0[pl.ds(r0, 1), :] += g_ref[pl.ds(at, 1), :]
                    acc1[pl.ds(r1, 1), :] += g_ref[pl.ds(at + 1, 1), :]
                return carry
            lax.fori_loop(0, block // group, add_group, 0)
        pl.when((step >= first) & (step < first + count))(add_block)
        first += count

    @pl.when(step == pl.num_programs(0) - 1)
    def _():
        def merge(i, carry):
            at = pl.ds(pl.multiple_of(i * 8, 8), 8)
            acc0[at, :] += acc1[at, :]
            return carry
        lax.fori_loop(0, padded // 8, merge, 0, unroll=8)
        copy = pltpu.make_async_copy(acc0.at[pl.ds(0, rows)], out_ref, sem)
        copy.start()
        copy.wait()


def scatter_rows(ids, grads, rows, init=None, block=2048):
    width = grads[0].shape[1]
    counts = [g.shape[0] // block for g in grads]
    total = sum(counts)
    starts = [sum(counts[:i]) for i in range(len(counts))]
    at = [lambda i, f=f, c=c: jnp.clip(i - f, 0, c - 1) for f, c in zip(starts, counts)]
    in_specs = [pl.BlockSpec((1, 1, block), lambda i, m=m: (m(i), 0, 0), memory_space=pltpu.SMEM) for m in at]
    in_specs += [pl.BlockSpec((block, width), lambda i, m=m: (m(i), 0)) for m in at]
    args = [v.reshape(-1, 1, block) for v in ids] + list(grads)
    has_init = init is not None
    if has_init:
        in_specs.append(pl.BlockSpec(memory_space=pl.ANY))
        args.append(init)
    return pl.pallas_call(
        functools.partial(scatter_kernel, has_init, rows, block, counts),
        grid=(total,),
        in_specs=in_specs,
        out_specs=pl.BlockSpec(memory_space=pl.ANY),
        out_shape=jax.ShapeDtypeStruct((rows, width), F32),
        scratch_shapes=[pltpu.VMEM((rows + 8, width), F32), pltpu.VMEM((rows + 8, width), F32), pltpu.SemaphoreType.DMA],
        compiler_params=pltpu.CompilerParams(dimension_semantics=("arbitrary",), vmem_limit_bytes=40 * 1024 * 1024),
        cost_estimate=pl.CostEstimate(flops=total * block * 3000000, bytes_accessed=8 * total * block * width, transcendentals=0),
        name="scatter_rows",
    )(*args)


def solution(mesh):
    arg_specs = (P('dp', None), P('tp', None), P(None), P(None), P(None), P(None), P(None, 'tp', None, None), P('tp', None, None), P('tp', None, None), P(None), P(None, 'tp'), P('tp'), P('tp', None), P(None), P('dp', None, None))
    out_specs = (P('dp', None, None), P('tp', 'dp'), P('dp'), P('dp'), P('dp'), P('dp'), P('dp', 'tp', None, None), P(('tp', 'dp')), P('tp', None, 'dp'), P('dp'), P('dp', 'tp'), P(('tp', 'dp')), P('tp', 'dp'), P('dp'))
    n_dp = mesh.shape['dp']

    def swap(val):
        return lax.ppermute(val, 'tp', [(0, 1), (1, 0)])

    def device_step(token_ids, embed_table, ln1_gain, ln1_bias, ln2_gain, ln2_bias, w_qkv, b_qkv, w_dense, b_dense, w_fc1, b_fc1, w_fc2, b_fc2, cotangent):
        n_seq, seq_len = token_ids.shape
        half_seq = n_seq // 2
        vocab_local, d_model = embed_table.shape
        heads_local, head_dim = w_qkv.shape[1], w_qkv.shape[3]
        attn_local = heads_local * head_dim
        ff_local = w_fc1.shape[1]
        tp_i, dp_i = lax.axis_index('tp'), lax.axis_index('dp')
        own_at, peer_at = tp_i * half_seq, (1 - tp_i) * half_seq
        zero = jnp.where(token_ids[0, 0] < 0, 1.0, 0.0).astype(F32)

        def from_peer(w):
            size = w.shape[0] // n_dp
            piece = swap(lax.dynamic_slice_in_dim(w, dp_i * size, size, 0).astype(F32))
            whole = lax.all_gather(piece, 'dp', axis=0, tiled=True)
            return (whole + zero).astype(BF16)

        def rows_of(ids):
            local = ids - tp_i * vocab_local
            ok = (local >= 0) & (local < vocab_local)
            picked = jnp.take(embed_table, jnp.where(ok, local, 0), axis=0)
            return jnp.where(ok[..., None], picked, jnp.zeros_like(picked)).astype(F32)

        ids_own = lax.dynamic_slice_in_dim(token_ids, own_at, half_seq, 0)
        ids_peer = lax.dynamic_slice_in_dim(token_ids, peer_at, half_seq, 0)
        bounds = []
        start = 0
        for size in CHUNKS:
            bounds.append((start, start + size))
            start += size
        sent_x = [swap(rows_of(ids_peer[a:b].reshape(-1))) for a, b in bounds]

        wqkv_own = w_qkv.transpose(2, 0, 1, 3).reshape(3 * d_model, attn_local)
        wqkv_peer = from_peer(wqkv_own)
        w_q, w_k, w_v = (jnp.concatenate([wqkv_own[i * d_model:(i + 1) * d_model], wqkv_peer[i * d_model:(i + 1) * d_model]], axis=1) for i in range(3))
        fc2_all = jnp.concatenate([w_fc2, from_peer(w_fc2)], axis=0)
        dense_own = w_dense.reshape(attn_local, d_model)
        dense_all = jnp.concatenate([dense_own, from_peer(dense_own)], axis=0)
        fc1_all = jnp.concatenate([w_fc1, from_peer(w_fc1)], axis=1)
        bqkv_own = b_qkv.transpose(1, 0, 2).reshape(-1)
        bias_own = jnp.concatenate([bqkv_own, b_fc1]).astype(F32)
        bias_peer = swap(bias_own)
        b_q, b_k, b_v = (jnp.concatenate([bias_own[i * attn_local:(i + 1) * attn_local], bias_peer[i * attn_local:(i + 1) * attn_local]]) for i in range(3))
        bfc1_all = jnp.concatenate([bias_own[3 * attn_local:], bias_peer[3 * attn_local:]])

        gain1, gain2 = ln1_gain.astype(F32), ln2_gain.astype(F32)
        shift1, shift2 = ln1_bias.astype(F32), ln2_bias.astype(F32)
        out_bias = b_dense.astype(F32) + b_fc2.astype(F32)
        consts = rope_consts(seq_len, head_dim)
        ids_all = lax.all_gather(token_ids, 'dp', axis=0)
        local_all = ids_all - tp_i * vocab_local
        local_all = jnp.where((local_all >= 0) & (local_all < vocab_local), local_all, vocab_local)
        local_own = lax.dynamic_slice_in_dim(local_all, own_at, half_seq, 1)
        local_peer = lax.dynamic_slice_in_dim(local_all, peer_at, half_seq, 1)
        cot_own = lax.dynamic_slice_in_dim(cotangent, own_at, half_seq, 0)

        layer_out = jnp.zeros(cotangent.shape, BF16)
        scatter_parts = []
        dw_sum = None
        after, held, older = None, [], []
        small_sum = None
        for (a, b), recv_x in zip(bounds, sent_x):
            tokens = (b - a) * seq_len
            flat = lambda v: v.reshape(tokens, v.shape[-1])
            cot = flat(cot_own[a:b])
            if after is not None:
                cot, recv_x, _ = lax.optimization_barrier((cot, recv_x, after + older))
                older = late
            grad_act = dot_f32(cot, fc2_all, ((1,), (1,))).astype(BF16)
            grad_ctx = dot_f32(cot, dense_all, ((1,), (1,))).astype(BF16)
            x = rows_of(ids_own[a:b].reshape(-1)) + recv_x
            centered = x - jnp.mean(x, axis=-1, keepdims=True)
            inv_std = lax.rsqrt(jnp.mean(centered * centered, axis=-1, keepdims=True) + EPS_NORM)
            normed = centered * inv_std
            hid1 = (normed * gain1 + shift1).astype(BF16)
            hid2 = (normed * gain2 + shift2).astype(BF16)
            q, k, v = ((dot_f32(hid1, w, ((1,), (0,))) + bias).astype(BF16).reshape(b - a, seq_len, -1) for w, bias in ((w_q, b_q), (w_k, b_k), (w_v, b_v)))
            ctx, d_q, d_k, d_v = (flat(r) for r in attention(q, k, v, grad_ctx.reshape(b - a, seq_len, -1), consts, head_dim))
            pre_low = (dot_f32(hid2, fc1_all, ((1,), (0,))) + bfc1_all).astype(BF16)
            grad_act, pre_low = lax.optimization_barrier((grad_act, pre_low))
            pre_act = pre_low.astype(F32)
            cdf = 0.5 + 0.5 * lax.erf(pre_act * HALF_ROOT)
            act = (pre_act * cdf).astype(BF16)
            slope = cdf + pre_act * (jnp.exp(-0.5 * pre_act * pre_act) * PDF_SCALE)
            grad_pre = (grad_act.astype(F32) * slope).astype(BF16)
            out_sum = x + dot_f32(ctx, dense_all, ((1,), (0,))) + dot_f32(act, fc2_all, ((1,), (0,)))
            recv_out = swap(out_sum)
            as_out = lambda v: (v + out_bias).astype(BF16).reshape(b - a, seq_len, d_model)
            layer_out = lax.dynamic_update_slice_in_dim(layer_out, as_out(out_sum), own_at + a, 0)
            layer_out = lax.dynamic_update_slice_in_dim(layer_out, as_out(recv_out), peer_at + a, 0)

            if held:
                out_sum, act, grad_pre, d_q, d_k, d_v, _ = lax.optimization_barrier((out_sum, act, grad_pre, d_q, d_k, d_v, held))
                held = []
            grad_h2 = dot_f32(grad_pre, fc1_all, ((1,), (1,))).astype(BF16).astype(F32)
            grad_h1 = (dot_f32(d_q, w_q, ((1,), (1,))) + dot_f32(d_k, w_k, ((1,), (1,))) + dot_f32(d_v, w_v, ((1,), (1,)))).astype(BF16).astype(F32)
            grad_norm = grad_h1 * gain1 + grad_h2 * gain2
            grad_x = cot.astype(F32) + inv_std * (grad_norm - jnp.mean(grad_norm, axis=-1, keepdims=True) - normed * jnp.mean(grad_norm * normed, axis=-1, keepdims=True))
            by_col = grad_x.reshape(tokens, n_dp, d_model // n_dp).transpose(1, 0, 2)
            mine = lax.all_to_all(by_col, 'dp', split_axis=0, concat_axis=0, tiled=True)
            theirs = swap(mine)
            after, held, late = [by_col, out_sum], [mine, recv_out], [theirs]
            scatter_parts.append((local_own[:, a:b].reshape(-1), mine.reshape(-1, d_model // n_dp), local_peer[:, a:b].reshape(-1), theirs.reshape(-1, d_model // n_dp)))

            if b == half_seq:
                hid1, hid2, ctx, act, grad_pre, d_q, d_k, d_v, _ = lax.optimization_barrier((hid1, hid2, ctx, act, grad_pre, d_q, d_k, d_v, by_col))
            t0 = ((0,), (0,))
            hid_fc1, pre_fc1 = hid2, grad_pre
            if b == half_seq:
                hid_fc1, pre_fc1, _ = lax.optimization_barrier((hid2, grad_pre, [mine, recv_out]))
            dws = [dot_f32(hid1, d_q, t0), dot_f32(hid1, d_k, t0), dot_f32(hid1, d_v, t0), dot_f32(ctx, cot, t0), dot_f32(hid_fc1, pre_fc1, t0), dot_f32(act, cot, t0)]
            total = lambda v: jnp.sum(v.astype(F32), axis=0)
            smalls = [total(grad_h1 * normed), total(grad_h1), total(grad_h2 * normed), total(grad_h2), total(cot), total(d_q), total(d_k), total(d_v), total(grad_pre)]
            dw_sum = dws if dw_sum is None else [p + r for p, r in zip(dw_sum, dws)]
            small_sum = smalls if small_sum is None else [p + r for p, r in zip(small_sum, smalls)]

        pick = lambda parts, i: [p for part in parts for p in (part[i], part[i + 2])]
        embed_first = scatter_rows(pick(scatter_parts[:-1], 0), pick(scatter_parts[:-1], 1), vocab_local)
        sum_embed = scatter_rows(pick(scatter_parts[-1:], 0), pick(scatter_parts[-1:], 1), vocab_local, embed_first)

        d_wq, d_wk, d_wv, d_dense, d_fc1, d_fc2 = dw_sum
        rs = lambda v, dim: lax.psum_scatter(v, 'dp', scatter_dimension=dim, tiled=True)
        r_fc2, r_fc1, r_dense = rs(d_fc2, 1), rs(d_fc1, 0), rs(d_dense, 1)
        r_q, r_k, r_v = rs(d_wq, 0), rs(d_wk, 0), rs(d_wv, 0)
        sum_fc2 = r_fc2[:ff_local] + swap(r_fc2[ff_local:])
        sum_fc1 = r_fc1[:, :ff_local] + swap(r_fc1[:, ff_local:])
        sum_dense = (r_dense[:attn_local] + swap(r_dense[attn_local:])).reshape(heads_local, head_dim, -1)
        own_qkv = jnp.stack([r[:, :attn_local].reshape(-1, heads_local, head_dim) for r in (r_q, r_k, r_v)], axis=2)
        peer_qkv = jnp.stack([r[:, attn_local:] for r in (r_q, r_k, r_v)])
        got_qkv = swap(peer_qkv).reshape(3, -1, heads_local, head_dim).transpose(1, 2, 0, 3)
        sum_qkv = own_qkv + got_qkv

        s_bqkv = [v.reshape(2, heads_local, head_dim) for v in small_sum[5:8]]
        bqkv_grad = jnp.stack(s_bqkv, axis=2)
        fc1_bias = small_sum[8].reshape(2, -1)
        pieces = small_sum[:5] + [bqkv_grad[0].reshape(-1), fc1_bias[0], bqkv_grad[1].reshape(-1), fc1_bias[1]]
        packed = jnp.concatenate([p.reshape(n_dp, -1) for p in pieces], axis=1)
        got = rs(packed, 0)[0]
        n_common = 5 * d_model // n_dp
        n_side = (3 * attn_local + ff_local) // n_dp
        common, side_own, side_peer = got[:n_common], got[n_common:n_common + n_side], got[n_common + n_side:]
        moved = swap(jnp.concatenate([common, side_peer]))
        common = (common + moved[:n_common]).reshape(5, -1)
        side = side_own + moved[n_common:]
        sum_bqkv, sum_bfc1 = side[:3 * attn_local // n_dp], side[3 * attn_local // n_dp:]
        return (layer_out, sum_embed, common[0], common[1], common[2], common[3], sum_qkv, sum_bqkv, sum_dense, common[4], sum_fc1, sum_bfc1, sum_fc2, common[4])

    return jax.shard_map(device_step, mesh=mesh, in_specs=arg_specs, out_specs=out_specs, check_vma=False)
```

```python
import functools
import jax
import jax.numpy as jnp
from jax import lax
from jax.experimental import pallas as pl
from jax.experimental.pallas import tpu as pltpu
from jax.sharding import PartitionSpec as P


EPS_NORM = 1e-5
ROPE_BASE = 10000.0
CHUNKS = (4, 6, 6)
SPILL = 64
HALF_ROOT = 0.5 ** 0.5
PDF_SCALE = (2.0 * 3.141592653589793) ** -0.5
F32, BF16 = jnp.float32, jnp.bfloat16


def dot_f32(a, b, dims):
    return lax.dot_general(a, b, (dims, ((), ())), preferred_element_type=F32)


def rope_consts(seq_len, head_dim):
    rot_dim = head_dim // 4
    half_rot = rot_dim // 2
    inv_freq = ROPE_BASE ** (-(jnp.arange(half_rot, dtype=F32) * 2.0) / rot_dim)
    angles = jnp.arange(seq_len, dtype=F32)[:, None] * inv_freq[None, :]
    angles = jnp.concatenate([angles, angles], axis=-1)
    rest = (seq_len, head_dim - rot_dim)
    cos_head = jnp.concatenate([jnp.cos(angles), jnp.ones(rest, F32)], axis=-1)
    sin_head = jnp.concatenate([jnp.sin(angles), jnp.zeros(rest, F32)], axis=-1)
    row = jnp.arange(2 * head_dim)[:, None]
    col = jnp.arange(2 * head_dim)[None, :]
    ch = col % head_dim
    turn = jnp.where((ch < half_rot) & (row == col + half_rot), -1.0, 0.0) + jnp.where((ch >= half_rot) & (ch < rot_dim) & (row == col - half_rot), 1.0, 0.0)
    return jnp.tile(cos_head, (1, 2)), jnp.tile(sin_head, (1, 2)), turn.astype(BF16)


def attention_kernel(head_dim, qkv_ref, g_ref, cos_ref, sin_ref, turn_ref, ctx_ref, dqkv_ref):
    seq_len, width = g_ref.shape[1], g_ref.shape[2]
    pair = 2 * head_dim
    scale = head_dim ** -0.5
    cos, sin, turn = cos_ref[...], sin_ref[...], turn_ref[...]
    low = lax.broadcasted_iota(jnp.int32, (seq_len, pair), 1) < head_dim
    causal = lax.broadcasted_iota(jnp.int32, (seq_len, seq_len), 0) >= lax.broadcasted_iota(jnp.int32, (seq_len, seq_len), 1)

    def rotate(val):
        turned = dot_f32(val, turn, ((1,), (0,)))
        return (val.astype(F32) * cos + turned * sin).astype(BF16)

    def unrotate(grad):
        turned = dot_f32(grad, turn, ((1,), (1,)))
        return (grad.astype(F32) * cos + turned * sin).astype(BF16)

    def step(j, carry):
        cols = pl.ds(pl.multiple_of(j * pair, pair), pair)
        k_cols = pl.ds(pl.multiple_of(width + j * pair, pair), pair)
        v_cols = pl.ds(pl.multiple_of(2 * width + j * pair, pair), pair)
        q = rotate(qkv_ref[0, :, cols])
        k = rotate(qkv_ref[0, :, k_cols])
        v = qkv_ref[0, :, v_cols]
        g = g_ref[0, :, cols]
        parts = []
        for head in range(2):
            mine = low if head == 0 else jnp.logical_not(low)
            q_h = jnp.where(mine, q, jnp.zeros_like(q))
            g_h = jnp.where(mine, g, jnp.zeros_like(g))
            scores = dot_f32(q_h, k, ((1,), (1,))) * scale
            scores = jnp.where(causal, scores, -1e30)
            top = jnp.max(scores, axis=-1, keepdims=True)
            expo = jnp.exp(scores - top)
            soft = expo * (1.0 / jnp.sum(expo, axis=-1, keepdims=True))
            probs = soft.astype(BF16)
            ctx = dot_f32(probs, v, ((1,), (0,)))
            d_probs = dot_f32(g_h, v, ((1,), (1,))).astype(BF16).astype(F32)
            d_v = dot_f32(probs, g, ((0,), (0,)))
            inner = jnp.sum(soft * d_probs, axis=-1, keepdims=True)
            d_s = (soft * (d_probs - inner) * scale).astype(BF16)
            d_q = dot_f32(d_s, k, ((1,), (0,)))
            d_k = dot_f32(d_s, q, ((0,), (0,)))
            parts.append((ctx, d_q, d_k, d_v))
        ctx, d_q, d_k, d_v = (jnp.where(low, a, b).astype(BF16) for a, b in zip(*parts))
        ctx_ref[0, :, cols] = ctx
        dqkv_ref[0, :, cols] = unrotate(d_q)
        dqkv_ref[0, :, k_cols] = unrotate(d_k)
        dqkv_ref[0, :, v_cols] = d_v
        return carry

    lax.fori_loop(0, width // pair, step, 0)


def attention(qkv, g, consts, head_dim):
    n, seq_len, width = g.shape
    big = lambda w: pl.BlockSpec((1, seq_len, w), lambda i: (i, 0, 0))
    const = [pl.BlockSpec(c.shape, lambda i: (0, 0)) for c in consts]
    flops = n * (width // head_dim) * 12 * seq_len * seq_len * 2 * head_dim
    return pl.pallas_call(
        functools.partial(attention_kernel, head_dim),
        grid=(n,),
        in_specs=[big(3 * width), big(width)] + const,
        out_specs=[big(width), big(3 * width)],
        out_shape=[jax.ShapeDtypeStruct(g.shape, BF16), jax.ShapeDtypeStruct(qkv.shape, BF16)],
        compiler_params=pltpu.CompilerParams(dimension_semantics=("arbitrary",), vmem_limit_bytes=40 * 1024 * 1024),
        cost_estimate=pl.CostEstimate(flops=4 * flops, bytes_accessed=16 * g.size, transcendentals=0),
        name="attention",
    )(qkv, g, *consts)


def scatter_kernel(has_init, rows, block, counts, *refs):
    n_arr = len(counts)
    ids_refs, g_refs, rest = refs[:n_arr], refs[n_arr:2 * n_arr], refs[2 * n_arr:]
    if has_init:
        init_ref, out_ref, acc0, acc1, sem = rest
    else:
        out_ref, acc0, acc1, sem = rest
    step = pl.program_id(0)
    padded = acc0.shape[0]
    group = 32

    @pl.when(step == 0)
    def _():
        def clear(i, carry):
            at = pl.ds(pl.multiple_of(i * 8, 8), 8)
            acc1[at, :] = jnp.zeros((8, acc1.shape[1]), F32)
            if not has_init:
                acc0[at, :] = jnp.zeros((8, acc0.shape[1]), F32)
            return carry

        lax.fori_loop(0, padded // 8, clear, 0, unroll=8)
        if has_init:
            copy = pltpu.make_async_copy(init_ref, acc0.at[pl.ds(0, rows)], sem)
            copy.start()
            copy.wait()

    first = 0
    for ids_ref, g_ref, count in zip(ids_refs, g_refs, counts):
        def add_block(ids_ref=ids_ref, g_ref=g_ref):
            def add_group(i, carry):
                for u in range(0, group, 2):
                    at = i * group + u
                    r0 = ids_ref[0, 0, at]
                    r1 = ids_ref[0, 0, at + 1]
                    acc0[pl.ds(r0, 1), :] += g_ref[pl.ds(at, 1), :]
                    acc1[pl.ds(r1, 1), :] += g_ref[pl.ds(at + 1, 1), :]
                return carry

            lax.fori_loop(0, block // group, add_group, 0)

        pl.when((step >= first) & (step < first + count))(add_block)
        first += count

    @pl.when(step == pl.num_programs(0) - 1)
    def _():
        def merge(i, carry):
            at = pl.ds(pl.multiple_of(i * 8, 8), 8)
            acc0[at, :] += acc1[at, :]
            return carry

        lax.fori_loop(0, padded // 8, merge, 0, unroll=8)
        copy = pltpu.make_async_copy(acc0.at[pl.ds(0, rows)], out_ref, sem)
        copy.start()
        copy.wait()


def scatter_rows(ids, grads, rows, init=None, block=2048):
    width = grads[0].shape[1]
    counts = [g.shape[0] // block for g in grads]
    total = sum(counts)
    starts = [sum(counts[:i]) for i in range(len(counts))]
    at = [lambda i, f=f, c=c: jnp.clip(i - f, 0, c - 1) for f, c in zip(starts, counts)]
    in_specs = [pl.BlockSpec((1, 1, block), lambda i, m=m: (m(i), 0, 0), memory_space=pltpu.SMEM) for m in at]
    in_specs += [pl.BlockSpec((block, width), lambda i, m=m: (m(i), 0)) for m in at]
    args = [v.reshape(-1, 1, block) for v in ids] + list(grads)
    has_init = init is not None
    if has_init:
        in_specs.append(pl.BlockSpec(memory_space=pl.ANY))
        args.append(init)
    return pl.pallas_call(
        functools.partial(scatter_kernel, has_init, rows, block, counts),
        grid=(total,),
        in_specs=in_specs,
        out_specs=pl.BlockSpec(memory_space=pl.ANY),
        out_shape=jax.ShapeDtypeStruct((rows, width), F32),
        scratch_shapes=[pltpu.VMEM((rows + SPILL, width), F32), pltpu.VMEM((rows + SPILL, width), F32), pltpu.SemaphoreType.DMA],
        compiler_params=pltpu.CompilerParams(dimension_semantics=("arbitrary",), vmem_limit_bytes=40 * 1024 * 1024),
        cost_estimate=pl.CostEstimate(flops=total * block * 3000000, bytes_accessed=8 * total * block * width, transcendentals=0),
        name="scatter_rows",
    )(*args)


def solution(mesh):
    arg_specs = (P('dp', None), P('tp', None), P(None), P(None), P(None), P(None), P(None, 'tp', None, None), P('tp', None, None), P('tp', None, None), P(None), P(None, 'tp'), P('tp'), P('tp', None), P(None), P('dp', None, None))
    out_specs = (P('dp', None, None), P('tp', 'dp'), P('dp'), P('dp'), P('dp'), P('dp'), P('dp', 'tp', None, None), P(('tp', 'dp')), P('tp', None, 'dp'), P('dp'), P('dp', 'tp'), P(('tp', 'dp')), P('tp', 'dp'), P('dp'))
    n_dp = mesh.shape['dp']

    def swap(val):
        return lax.ppermute(val, 'tp', [(0, 1), (1, 0)])

    def device_step(token_ids, embed_table, ln1_gain, ln1_bias, ln2_gain, ln2_bias, w_qkv, b_qkv, w_dense, b_dense, w_fc1, b_fc1, w_fc2, b_fc2, cotangent):
        n_seq, seq_len = token_ids.shape
        half_seq = n_seq // 2
        vocab_local, d_model = embed_table.shape
        heads_local, head_dim = w_qkv.shape[1], w_qkv.shape[3]
        attn_local = heads_local * head_dim
        ff_local = w_fc1.shape[1]
        tp_i, dp_i = lax.axis_index('tp'), lax.axis_index('dp')
        own_at, peer_at = tp_i * half_seq, (1 - tp_i) * half_seq
        zero = jnp.where(token_ids[0, 0] < 0, 1.0, 0.0).astype(F32)

        def from_peer(w):
            size = w.shape[0] // n_dp
            piece = swap(lax.dynamic_slice_in_dim(w, dp_i * size, size, 0).astype(F32))
            piece, _ = lax.optimization_barrier((piece, first_rows))
            whole = lax.all_gather(piece, 'dp', axis=0, tiled=True)
            return (whole + zero).astype(BF16)

        def rows_of(ids):
            local = ids - tp_i * vocab_local
            ok = (local >= 0) & (local < vocab_local)
            other = jnp.where(local < 0, local + vocab_local, local - vocab_local)
            picked = jnp.take(embed_table, jnp.where(ok, local, other), axis=0, mode='clip')
            return jnp.where(ok[..., None], picked, jnp.zeros_like(picked)).astype(F32)

        ids_own = lax.dynamic_slice_in_dim(token_ids, own_at, half_seq, 0)
        ids_peer = lax.dynamic_slice_in_dim(token_ids, peer_at, half_seq, 0)
        bounds = []
        start = 0
        for size in CHUNKS:
            bounds.append((start, start + size))
            start += size
        first_rows = rows_of(ids_peer[bounds[0][0]:bounds[0][1]].reshape(-1))
        sent_x = [swap(first_rows)] + [swap(rows_of(ids_peer[a:b].reshape(-1))) for a, b in bounds[1:]]

        wqkv_own = w_qkv.transpose(2, 0, 1, 3).reshape(3 * d_model, attn_local)
        wqkv_peer = from_peer(wqkv_own)
        qkv_all = jnp.concatenate([w[i * d_model:(i + 1) * d_model] for i in range(3) for w in (wqkv_own, wqkv_peer)], axis=1)
        dense_own = w_dense.reshape(attn_local, d_model)
        dense_all = jnp.concatenate([dense_own, from_peer(dense_own)], axis=0)
        fc1_all = jnp.concatenate([w_fc1, from_peer(w_fc1)], axis=1)
        fc2_all = jnp.concatenate([w_fc2, from_peer(w_fc2)], axis=0)
        bqkv_own = b_qkv.transpose(1, 0, 2).reshape(-1)
        bias_own = jnp.concatenate([bqkv_own, b_fc1]).astype(F32)
        bias_peer = swap(bias_own)
        bqkv_all = jnp.concatenate([v[i * attn_local:(i + 1) * attn_local] for i in range(3) for v in (bias_own, bias_peer)])
        bfc1_all = jnp.concatenate([bias_own[3 * attn_local:], bias_peer[3 * attn_local:]])

        gain1, gain2 = ln1_gain.astype(F32), ln2_gain.astype(F32)
        shift1, shift2 = ln1_bias.astype(F32), ln2_bias.astype(F32)
        out_bias = b_dense.astype(F32) + b_fc2.astype(F32)
        consts = rope_consts(seq_len, head_dim)
        ids_all = lax.all_gather(token_ids, 'dp', axis=0)
        local_all = ids_all - tp_i * vocab_local
        spread = vocab_local + lax.broadcasted_iota(jnp.int32, local_all.shape, 2) % SPILL
        local_all = jnp.where((local_all >= 0) & (local_all < vocab_local), local_all, spread)
        local_own = lax.dynamic_slice_in_dim(local_all, own_at, half_seq, 1)
        local_peer = lax.dynamic_slice_in_dim(local_all, peer_at, half_seq, 1)
        cot_own = lax.dynamic_slice_in_dim(cotangent, own_at, half_seq, 0)

        layer_out = jnp.zeros(cotangent.shape, BF16)
        scatter_parts = []
        dw_sum = small_sum = None
        t0 = ((0,), (0,))
        total = lambda v: jnp.sum(v.astype(F32), axis=0)
        after, held, older = [], [], []
        for (a, b), recv_x in zip(bounds, sent_x):
            last = b == half_seq
            tokens = (b - a) * seq_len
            flat = lambda v: v.reshape(tokens, v.shape[-1])
            cube = lambda v: v.reshape(b - a, seq_len, v.shape[-1])
            cot = flat(cot_own[a:b])
            if after:
                cot, recv_x, _ = lax.optimization_barrier((cot, recv_x, after))
            grad_act = dot_f32(cot, fc2_all, ((1,), (1,))).astype(BF16)
            grad_ctx = dot_f32(cot, dense_all, ((1,), (1,))).astype(BF16)
            x = rows_of(ids_own[a:b].reshape(-1)) + recv_x
            centered = x - jnp.mean(x, axis=-1, keepdims=True)
            inv_std = lax.rsqrt(jnp.mean(centered * centered, axis=-1, keepdims=True) + EPS_NORM)
            normed = centered * inv_std
            hid1 = (normed * gain1 + shift1).astype(BF16)
            hid2 = (normed * gain2 + shift2).astype(BF16)
            qkv = (dot_f32(hid1, qkv_all, ((1,), (0,))) + bqkv_all).astype(BF16)
            pre_low = (dot_f32(hid2, fc1_all, ((1,), (0,))) + bfc1_all).astype(BF16)
            grad_act, pre_low = lax.optimization_barrier((grad_act, pre_low))
            ctx, d_qkv = (flat(r) for r in attention(cube(qkv), cube(grad_ctx), consts, head_dim))
            pre_act = pre_low.astype(F32)
            cdf = 0.5 + 0.5 * lax.erf(pre_act * HALF_ROOT)
            act = (pre_act * cdf).astype(BF16)
            slope = cdf + pre_act * (jnp.exp(-0.5 * pre_act * pre_act) * PDF_SCALE)
            grad_pre = (grad_act.astype(F32) * slope).astype(BF16)
            out_sum = x + dot_f32(ctx, dense_all, ((1,), (0,))) + dot_f32(act, fc2_all, ((1,), (0,)))
            recv_out = swap(out_sum)
            d_fc2, d_dense = dot_f32(act, cot, t0), dot_f32(ctx, cot, t0)
            if dw_sum is not None:
                d_fc2, d_dense = dw_sum[0] + d_fc2, dw_sum[1] + d_dense
            grad_pre, d_qkv, _ = lax.optimization_barrier((grad_pre, d_qkv, [out_sum, d_fc2, d_dense] + held))

            grad_h2 = dot_f32(grad_pre, fc1_all, ((1,), (1,))).astype(BF16).astype(F32)
            grad_h1 = dot_f32(d_qkv, qkv_all, ((1,), (1,))).astype(BF16).astype(F32)
            grad_norm = grad_h1 * gain1 + grad_h2 * gain2
            grad_x = cot.astype(F32) + inv_std * (grad_norm - jnp.mean(grad_norm, axis=-1, keepdims=True) - normed * jnp.mean(grad_norm * normed, axis=-1, keepdims=True))
            by_col = grad_x.reshape(tokens, n_dp, d_model // n_dp).transpose(1, 0, 2)
            mine = lax.all_to_all(by_col, 'dp', split_axis=0, concat_axis=0, tiled=True)
            theirs = swap(mine)
            scatter_parts.append((local_own[:, a:b].reshape(-1), mine.reshape(-1, d_model // n_dp), local_peer[:, a:b].reshape(-1), theirs.reshape(-1, d_model // n_dp)))

            hid1, hid2, grad_pre, d_qkv, _ = lax.optimization_barrier((hid1, hid2, grad_pre, d_qkv, by_col))
            d_fc1 = dot_f32(hid2, grad_pre, t0)
            d_wqkv = dot_f32(hid1, d_qkv, t0)
            if dw_sum is not None:
                d_fc1, d_wqkv = dw_sum[2] + d_fc1, dw_sum[3] + d_wqkv
            dw_sum = [d_fc2, d_dense, d_fc1, d_wqkv]
            smalls = [total(grad_h1 * normed), total(grad_h1), total(grad_h2 * normed), total(grad_h2), total(cot), total(d_qkv), total(grad_pre)]
            small_sum = smalls if small_sum is None else [p + r for p, r in zip(small_sum, smalls)]
            after = [by_col, d_fc1, d_wqkv] + small_sum
            held, older = [mine] + older, [recv_out, theirs]
            as_out = lambda v: (v + out_bias).astype(BF16).reshape(b - a, seq_len, d_model)
            layer_out = lax.dynamic_update_slice_in_dim(layer_out, as_out(out_sum), own_at + a, 0)
            if last:
                last_out = (recv_out, a, as_out)
            else:
                layer_out = lax.dynamic_update_slice_in_dim(layer_out, as_out(recv_out), peer_at + a, 0)

        pick = lambda parts, i: [p for part in parts for p in (part[i], part[i + 2])]
        embed_first = scatter_rows(pick(scatter_parts[:-1], 0), pick(scatter_parts[:-1], 1), vocab_local)
        sum_embed = scatter_rows(pick(scatter_parts[-1:], 0), pick(scatter_parts[-1:], 1), vocab_local, embed_first)
        recv_out, a, as_out = last_out
        recv_out, _ = lax.optimization_barrier((recv_out, embed_first[:8]))
        layer_out = lax.dynamic_update_slice_in_dim(layer_out, as_out(recv_out), peer_at + a, 0)

        d_fc2, d_dense, d_fc1, d_wqkv = dw_sum
        rs = lambda v, dim: lax.psum_scatter(v, 'dp', scatter_dimension=dim, tiled=True)
        r_fc2 = rs(d_fc2, 1)
        r_dense = rs(d_dense, 1)
        r_fc1 = rs(d_fc1, 0)
        r_qkv = rs(d_wqkv, 0)
        r_qkv = r_qkv.reshape(-1, 3, 2, heads_local, head_dim)
        got = [swap(r_fc2[ff_local:]), swap(r_dense[attn_local:]), swap(r_fc1[:, ff_local:]), swap(r_qkv[:, :, 1].reshape(-1, 3 * attn_local))]
        got, _ = lax.optimization_barrier((got, sum_embed[:8]))
        sum_fc2 = r_fc2[:ff_local] + got[0]
        sum_dense = (r_dense[:attn_local] + got[1]).reshape(heads_local, head_dim, -1)
        sum_fc1 = r_fc1[:, :ff_local] + got[2]
        sum_qkv = (r_qkv[:, :, 0] + got[3].reshape(-1, 3, heads_local, head_dim)).transpose(0, 2, 1, 3)

        bqkv_grad = small_sum[5].reshape(3, 2, heads_local, head_dim).transpose(1, 2, 0, 3).reshape(2, -1)
        side = jnp.concatenate([bqkv_grad, small_sum[6].reshape(2, -1)], axis=1)
        side = jnp.where(tp_i == 0, side, side[::-1])
        packed = lax.psum(jnp.concatenate(small_sum[:5] + [side[0], side[1]]), ('tp', 'dp'))
        piece = d_model // n_dp
        common = [lax.dynamic_slice_in_dim(packed, i * d_model + dp_i * piece, piece, 0) for i in range(5)]
        base = 5 * d_model + tp_i * side.shape[1]
        n_b, n_f = 3 * attn_local // n_dp, ff_local // n_dp
        sum_bqkv = lax.dynamic_slice_in_dim(packed, base + dp_i * n_b, n_b, 0)
        sum_bfc1 = lax.dynamic_slice_in_dim(packed, base + 3 * attn_local + dp_i * n_f, n_f, 0)
        return (layer_out, sum_embed, common[0], common[1], common[2], common[3], sum_qkv, sum_bqkv, sum_dense, common[4], sum_fc1, sum_bfc1, sum_fc2, common[4])

    return jax.shard_map(device_step, mesh=mesh, in_specs=arg_specs, out_specs=out_specs, check_vma=False)
```

```python
import functools
import jax
import jax.numpy as jnp
from jax import lax
from jax.experimental import pallas as pl
from jax.experimental.pallas import tpu as pltpu
from jax.sharding import PartitionSpec as P


EPS_NORM = 1e-5
ROPE_BASE = 10000.0
CHUNKS = (4, 6, 6)
SPILL = 64
HALF_ROOT = 0.5 ** 0.5
PDF_SCALE = (2.0 * 3.141592653589793) ** -0.5
F32, BF16 = jnp.float32, jnp.bfloat16


def dot_f32(a, b, dims):
    return lax.dot_general(a, b, (dims, ((), ())), preferred_element_type=F32)


def rope_consts(seq_len, head_dim):
    rot_dim = head_dim // 4
    half_rot = rot_dim // 2
    inv_freq = ROPE_BASE ** (-(jnp.arange(half_rot, dtype=F32) * 2.0) / rot_dim)
    angles = jnp.arange(seq_len, dtype=F32)[:, None] * inv_freq[None, :]
    angles = jnp.concatenate([angles, angles], axis=-1)
    rest = (seq_len, head_dim - rot_dim)
    cos_head = jnp.concatenate([jnp.cos(angles), jnp.ones(rest, F32)], axis=-1)
    sin_head = jnp.concatenate([jnp.sin(angles), jnp.zeros(rest, F32)], axis=-1)
    row = jnp.arange(2 * head_dim)[:, None]
    col = jnp.arange(2 * head_dim)[None, :]
    ch = col % head_dim
    turn = jnp.where((ch < half_rot) & (row == col + half_rot), -1.0, 0.0) + jnp.where((ch >= half_rot) & (ch < rot_dim) & (row == col - half_rot), 1.0, 0.0)
    return jnp.tile(cos_head, (1, 2)), jnp.tile(sin_head, (1, 2)), turn.astype(BF16)


def attention_kernel(head_dim, qkv_ref, g_ref, cos_ref, sin_ref, turn_ref, ctx_ref, dqkv_ref):
    seq_len, width = g_ref.shape[1], g_ref.shape[2]
    pair = 2 * head_dim
    scale = head_dim ** -0.5
    cos, sin, turn = cos_ref[...], sin_ref[...], turn_ref[...]
    low = lax.broadcasted_iota(jnp.int32, (seq_len, pair), 1) < head_dim
    causal = lax.broadcasted_iota(jnp.int32, (seq_len, seq_len), 0) >= lax.broadcasted_iota(jnp.int32, (seq_len, seq_len), 1)

    def rotate(val):
        turned = dot_f32(val, turn, ((1,), (0,)))
        return (val.astype(F32) * cos + turned * sin).astype(BF16)

    def unrotate(grad):
        turned = dot_f32(grad, turn, ((1,), (1,)))
        return (grad.astype(F32) * cos + turned * sin).astype(BF16)

    def step(j, carry):
        cols = pl.ds(pl.multiple_of(j * pair, pair), pair)
        k_cols = pl.ds(pl.multiple_of(width + j * pair, pair), pair)
        v_cols = pl.ds(pl.multiple_of(2 * width + j * pair, pair), pair)
        q = rotate(qkv_ref[0, :, cols])
        k = rotate(qkv_ref[0, :, k_cols])
        v = qkv_ref[0, :, v_cols]
        g = g_ref[0, :, cols]
        parts = []
        for head in range(2):
            mine = low if head == 0 else jnp.logical_not(low)
            q_h = jnp.where(mine, q, jnp.zeros_like(q))
            g_h = jnp.where(mine, g, jnp.zeros_like(g))
            scores = dot_f32(q_h, k, ((1,), (1,))) * scale
            scores = jnp.where(causal, scores, -1e30)
            top = jnp.max(scores, axis=-1, keepdims=True)
            expo = jnp.exp(scores - top)
            soft = expo * (1.0 / jnp.sum(expo, axis=-1, keepdims=True))
            probs = soft.astype(BF16)
            ctx = dot_f32(probs, v, ((1,), (0,)))
            d_probs = dot_f32(g_h, v, ((1,), (1,))).astype(BF16).astype(F32)
            d_v = dot_f32(probs, g, ((0,), (0,)))
            inner = jnp.sum(soft * d_probs, axis=-1, keepdims=True)
            d_s = (soft * (d_probs - inner) * scale).astype(BF16)
            d_q = dot_f32(d_s, k, ((1,), (0,)))
            d_k = dot_f32(d_s, q, ((0,), (0,)))
            parts.append((ctx, d_q, d_k, d_v))
        ctx, d_q, d_k, d_v = (jnp.where(low, a, b).astype(BF16) for a, b in zip(*parts))
        ctx_ref[0, :, cols] = ctx
        dqkv_ref[0, :, cols] = unrotate(d_q)
        dqkv_ref[0, :, k_cols] = unrotate(d_k)
        dqkv_ref[0, :, v_cols] = d_v
        return carry

    lax.fori_loop(0, width // pair, step, 0)


def attention(qkv, g, consts, head_dim):
    n, seq_len, width = g.shape
    big = lambda w: pl.BlockSpec((1, seq_len, w), lambda i: (i, 0, 0))
    const = [pl.BlockSpec(c.shape, lambda i: (0, 0)) for c in consts]
    flops = n * (width // head_dim) * 12 * seq_len * seq_len * 2 * head_dim
    return pl.pallas_call(
        functools.partial(attention_kernel, head_dim),
        grid=(n,),
        in_specs=[big(3 * width), big(width)] + const,
        out_specs=[big(width), big(3 * width)],
        out_shape=[jax.ShapeDtypeStruct(g.shape, BF16), jax.ShapeDtypeStruct(qkv.shape, BF16)],
        compiler_params=pltpu.CompilerParams(dimension_semantics=("arbitrary",), vmem_limit_bytes=40 * 1024 * 1024),
        cost_estimate=pl.CostEstimate(flops=4 * flops, bytes_accessed=16 * g.size, transcendentals=0),
        name="attention",
    )(qkv, g, *consts)


def scatter_kernel(has_init, rows, block, counts, *refs):
    n_arr = len(counts)
    ids_refs, g_refs, rest = refs[:n_arr], refs[n_arr:2 * n_arr], refs[2 * n_arr:]
    if has_init:
        init_ref, out_ref, acc0, acc1, sem = rest
    else:
        out_ref, acc0, acc1, sem = rest
    step = pl.program_id(0)
    padded = acc0.shape[0]
    group = 32

    @pl.when(step == 0)
    def _():
        def clear(i, carry):
            at = pl.ds(pl.multiple_of(i * 8, 8), 8)
            acc1[at, :] = jnp.zeros((8, acc1.shape[1]), F32)
            if not has_init:
                acc0[at, :] = jnp.zeros((8, acc0.shape[1]), F32)
            return carry

        lax.fori_loop(0, padded // 8, clear, 0, unroll=8)
        if has_init:
            copy = pltpu.make_async_copy(init_ref, acc0.at[pl.ds(0, rows)], sem)
            copy.start()
            copy.wait()

    first = 0
    for ids_ref, g_ref, count in zip(ids_refs, g_refs, counts):
        def add_block(ids_ref=ids_ref, g_ref=g_ref):
            def add_group(i, carry):
                for u in range(0, group, 2):
                    at = i * group + u
                    r0 = ids_ref[0, 0, at]
                    r1 = ids_ref[0, 0, at + 1]
                    acc0[pl.ds(r0, 1), :] += g_ref[pl.ds(at, 1), :]
                    acc1[pl.ds(r1, 1), :] += g_ref[pl.ds(at + 1, 1), :]
                return carry

            lax.fori_loop(0, block // group, add_group, 0)

        pl.when((step >= first) & (step < first + count))(add_block)
        first += count

    @pl.when(step == pl.num_programs(0) - 1)
    def _():
        def merge(i, carry):
            at = pl.ds(pl.multiple_of(i * 8, 8), 8)
            acc0[at, :] += acc1[at, :]
            return carry

        lax.fori_loop(0, padded // 8, merge, 0, unroll=8)
        copy = pltpu.make_async_copy(acc0.at[pl.ds(0, rows)], out_ref, sem)
        copy.start()
        copy.wait()


def scatter_rows(ids, grads, rows, init=None, block=2048):
    width = grads[0].shape[1]
    counts = [g.shape[0] // block for g in grads]
    total = sum(counts)
    starts = [sum(counts[:i]) for i in range(len(counts))]
    at = [lambda i, f=f, c=c: jnp.clip(i - f, 0, c - 1) for f, c in zip(starts, counts)]
    in_specs = [pl.BlockSpec((1, 1, block), lambda i, m=m: (m(i), 0, 0), memory_space=pltpu.SMEM) for m in at]
    in_specs += [pl.BlockSpec((block, width), lambda i, m=m: (m(i), 0)) for m in at]
    args = [v.reshape(-1, 1, block) for v in ids] + list(grads)
    has_init = init is not None
    if has_init:
        in_specs.append(pl.BlockSpec(memory_space=pl.ANY))
        args.append(init)
    return pl.pallas_call(
        functools.partial(scatter_kernel, has_init, rows, block, counts),
        grid=(total,),
        in_specs=in_specs,
        out_specs=pl.BlockSpec(memory_space=pl.ANY),
        out_shape=jax.ShapeDtypeStruct((rows, width), F32),
        scratch_shapes=[pltpu.VMEM((rows + SPILL, width), F32), pltpu.VMEM((rows + SPILL, width), F32), pltpu.SemaphoreType.DMA],
        compiler_params=pltpu.CompilerParams(dimension_semantics=("arbitrary",), vmem_limit_bytes=40 * 1024 * 1024),
        cost_estimate=pl.CostEstimate(flops=total * block * 3000000, bytes_accessed=8 * total * block * width, transcendentals=0),
        name="scatter_rows",
    )(*args)


def solution(mesh):
    arg_specs = (P('dp', None), P('tp', None), P(None), P(None), P(None), P(None), P(None, 'tp', None, None), P('tp', None, None), P('tp', None, None), P(None), P(None, 'tp'), P('tp'), P('tp', None), P(None), P('dp', None, None))
    out_specs = (P('dp', None, None), P('tp', 'dp'), P('dp'), P('dp'), P('dp'), P('dp'), P('dp', 'tp', None, None), P(('tp', 'dp')), P('tp', None, 'dp'), P('dp'), P('dp', 'tp'), P(('tp', 'dp')), P('tp', 'dp'), P('dp'))
    n_dp = mesh.shape['dp']

    def swap(val):
        return lax.ppermute(val, 'tp', [(0, 1), (1, 0)])

    def device_step(token_ids, embed_table, ln1_gain, ln1_bias, ln2_gain, ln2_bias, w_qkv, b_qkv, w_dense, b_dense, w_fc1, b_fc1, w_fc2, b_fc2, cotangent):
        n_seq, seq_len = token_ids.shape
        half_seq = n_seq // 2
        vocab_local, d_model = embed_table.shape
        heads_local, head_dim = w_qkv.shape[1], w_qkv.shape[3]
        attn_local = heads_local * head_dim
        ff_local = w_fc1.shape[1]
        tp_i, dp_i = lax.axis_index('tp'), lax.axis_index('dp')
        own_at, peer_at = tp_i * half_seq, (1 - tp_i) * half_seq
        zero = jnp.where(token_ids[0, 0] < 0, 1.0, 0.0).astype(F32)

        def from_peer(w, ready):
            size = w.shape[0] // n_dp
            piece = swap(lax.dynamic_slice_in_dim(w, dp_i * size, size, 0).astype(F32))
            piece, _ = lax.optimization_barrier((piece, ready))
            whole = lax.all_gather(piece, 'dp', axis=0, tiled=True)
            return (whole + zero).astype(BF16)

        def pick_rows(ids):
            local = ids - tp_i * vocab_local
            ok = (local >= 0) & (local < vocab_local)
            other = jnp.where(local < 0, local + vocab_local, local - vocab_local)
            picked = jnp.take(embed_table, jnp.where(ok, local, other), axis=0, mode='clip')
            return picked, ok

        def rows_of(picked, ok):
            return jnp.where(ok[..., None], picked, jnp.zeros_like(picked)).astype(F32)

        ids_own = lax.dynamic_slice_in_dim(token_ids, own_at, half_seq, 0)
        ids_peer = lax.dynamic_slice_in_dim(token_ids, peer_at, half_seq, 0)
        bounds = []
        start = 0
        for size in CHUNKS:
            bounds.append((start, start + size))
            start += size
        first_rows = rows_of(*pick_rows(ids_peer[bounds[0][0]:bounds[0][1]].reshape(-1)))
        sent_x = [swap(first_rows)] + [swap(rows_of(*pick_rows(ids_peer[a:b].reshape(-1)))) for a, b in bounds[1:]]
        picked_own = [pick_rows(ids_own[a:b].reshape(-1)) for a, b in bounds]

        wqkv_own = w_qkv.transpose(2, 0, 1, 3).reshape(3 * d_model, attn_local)
        wqkv_peer = from_peer(wqkv_own, first_rows)
        qkv_all = jnp.concatenate([w[i * d_model:(i + 1) * d_model] for i in range(3) for w in (wqkv_own, wqkv_peer)], axis=1)
        dense_own = w_dense.reshape(attn_local, d_model)
        dense_all = jnp.concatenate([dense_own, from_peer(dense_own, first_rows)], axis=0)
        fc1_all = jnp.concatenate([w_fc1, from_peer(w_fc1, [p for p, _ in picked_own])], axis=1)
        fc2_all = jnp.concatenate([w_fc2, from_peer(w_fc2, first_rows)], axis=0)
        bqkv_own = b_qkv.transpose(1, 0, 2).reshape(-1)
        bias_own = jnp.concatenate([bqkv_own, b_fc1]).astype(F32)
        bias_peer = swap(bias_own)
        bqkv_all = jnp.concatenate([v[i * attn_local:(i + 1) * attn_local] for i in range(3) for v in (bias_own, bias_peer)])
        bfc1_all = jnp.concatenate([bias_own[3 * attn_local:], bias_peer[3 * attn_local:]])

        gain1, gain2 = ln1_gain.astype(F32), ln2_gain.astype(F32)
        shift1, shift2 = ln1_bias.astype(F32), ln2_bias.astype(F32)
        out_bias = b_dense.astype(F32) + b_fc2.astype(F32)
        consts = rope_consts(seq_len, head_dim)
        ids_all = lax.all_gather(token_ids, 'dp', axis=0)
        local_all = ids_all - tp_i * vocab_local
        spread = vocab_local + lax.broadcasted_iota(jnp.int32, local_all.shape, 2) % SPILL
        local_all = jnp.where((local_all >= 0) & (local_all < vocab_local), local_all, spread)
        local_own = lax.dynamic_slice_in_dim(local_all, own_at, half_seq, 1)
        local_peer = lax.dynamic_slice_in_dim(local_all, peer_at, half_seq, 1)
        cot_own = lax.dynamic_slice_in_dim(cotangent, own_at, half_seq, 0)

        layer_out = jnp.zeros(cotangent.shape, BF16)
        scatter_parts = []
        dw_sum = small_sum = None
        t0 = ((0,), (0,))
        total = lambda v: jnp.sum(v.astype(F32), axis=0)
        after, held, older = [], [], []
        for c, ((a, b), recv_x) in enumerate(zip(bounds, sent_x)):
            last = b == half_seq
            tokens = (b - a) * seq_len
            flat = lambda v: v.reshape(tokens, v.shape[-1])
            cube = lambda v: v.reshape(b - a, seq_len, v.shape[-1])
            cot = flat(cot_own[a:b])
            if after:
                cot, recv_x, _ = lax.optimization_barrier((cot, recv_x, after))
            if c == 0:
                recv_x, local_own, local_peer = lax.optimization_barrier((recv_x, local_own, local_peer))
            grad_act = dot_f32(cot, fc2_all, ((1,), (1,))).astype(BF16)
            grad_ctx = dot_f32(cot, dense_all, ((1,), (1,))).astype(BF16)
            x = rows_of(*picked_own[c]) + recv_x
            centered = x - jnp.mean(x, axis=-1, keepdims=True)
            inv_std = lax.rsqrt(jnp.mean(centered * centered, axis=-1, keepdims=True) + EPS_NORM)
            normed = centered * inv_std
            hid1 = (normed * gain1 + shift1).astype(BF16)
            hid2 = (normed * gain2 + shift2).astype(BF16)
            qkv = (dot_f32(hid1, qkv_all, ((1,), (0,))) + bqkv_all).astype(BF16)
            pre_low = (dot_f32(hid2, fc1_all, ((1,), (0,))) + bfc1_all).astype(BF16)
            grad_act, pre_low = lax.optimization_barrier((grad_act, pre_low))
            ctx, d_qkv = (flat(r) for r in attention(cube(qkv), cube(grad_ctx), consts, head_dim))
            pre_act = pre_low.astype(F32)
            cdf = 0.5 + 0.5 * lax.erf(pre_act * HALF_ROOT)
            act = (pre_act * cdf).astype(BF16)
            slope = cdf + pre_act * (jnp.exp(-0.5 * pre_act * pre_act) * PDF_SCALE)
            grad_pre = (grad_act.astype(F32) * slope).astype(BF16)
            out_sum = x + dot_f32(ctx, dense_all, ((1,), (0,))) + dot_f32(act, fc2_all, ((1,), (0,)))
            recv_out = swap(out_sum)
            d_fc2, d_dense = dot_f32(act, cot, t0), dot_f32(ctx, cot, t0)
            if dw_sum is not None:
                d_fc2, d_dense = dw_sum[0] + d_fc2, dw_sum[1] + d_dense
            grad_pre, d_qkv, _ = lax.optimization_barrier((grad_pre, d_qkv, [out_sum, d_fc2, d_dense] + held))

            grad_h2 = dot_f32(grad_pre, fc1_all, ((1,), (1,))).astype(BF16).astype(F32)
            grad_h1 = dot_f32(d_qkv, qkv_all, ((1,), (1,))).astype(BF16).astype(F32)
            grad_norm = grad_h1 * gain1 + grad_h2 * gain2
            grad_x = cot.astype(F32) + inv_std * (grad_norm - jnp.mean(grad_norm, axis=-1, keepdims=True) - normed * jnp.mean(grad_norm * normed, axis=-1, keepdims=True))
            by_col = grad_x.reshape(tokens, n_dp, d_model // n_dp).transpose(1, 0, 2)
            mine = lax.all_to_all(by_col, 'dp', split_axis=0, concat_axis=0, tiled=True)
            theirs = swap(mine)
            scatter_parts.append((local_own[:, a:b].reshape(-1), mine.reshape(-1, d_model // n_dp), local_peer[:, a:b].reshape(-1), theirs.reshape(-1, d_model // n_dp)))

            hid1, hid2, grad_pre, d_qkv, _ = lax.optimization_barrier((hid1, hid2, grad_pre, d_qkv, by_col))
            d_fc1 = dot_f32(hid2, grad_pre, t0)
            d_wqkv = dot_f32(hid1, d_qkv, t0)
            if dw_sum is not None:
                d_fc1, d_wqkv = dw_sum[2] + d_fc1, dw_sum[3] + d_wqkv
            dw_sum = [d_fc2, d_dense, d_fc1, d_wqkv]
            smalls = [total(grad_h1 * normed), total(grad_h1), total(grad_h2 * normed), total(grad_h2), total(cot), total(d_qkv), total(grad_pre)]
            small_sum = smalls if small_sum is None else [p + r for p, r in zip(small_sum, smalls)]
            after = [by_col, d_fc1, d_wqkv] + small_sum
            held, older = [mine] + older, [recv_out, theirs]
            as_out = lambda v: (v + out_bias).astype(BF16).reshape(b - a, seq_len, d_model)
            layer_out = lax.dynamic_update_slice_in_dim(layer_out, as_out(out_sum), own_at + a, 0)
            if last:
                last_out = (recv_out, a, as_out)
            else:
                layer_out = lax.dynamic_update_slice_in_dim(layer_out, as_out(recv_out), peer_at + a, 0)

        pick = lambda parts, i: [p for part in parts for p in (part[i], part[i + 2])]
        embed_first = scatter_rows(pick(scatter_parts[:-1], 0), pick(scatter_parts[:-1], 1), vocab_local)
        sum_embed = scatter_rows(pick(scatter_parts[-1:], 0), pick(scatter_parts[-1:], 1), vocab_local, embed_first)
        recv_out, a, as_out = last_out
        recv_out, _ = lax.optimization_barrier((recv_out, embed_first[:8]))
        layer_out = lax.dynamic_update_slice_in_dim(layer_out, as_out(recv_out), peer_at + a, 0)

        d_fc2, d_dense, d_fc1, d_wqkv = dw_sum
        rs = lambda v, dim: lax.psum_scatter(v, 'dp', scatter_dimension=dim, tiled=True)
        r_fc2 = rs(d_fc2, 1)
        r_dense = rs(d_dense, 1)
        r_fc1 = rs(d_fc1, 0)
        r_qkv = rs(d_wqkv, 0)
        r_qkv = r_qkv.reshape(-1, 3, 2, heads_local, head_dim)
        got = [swap(r_fc2[ff_local:]), swap(r_dense[attn_local:]), swap(r_fc1[:, ff_local:]), swap(r_qkv[:, :, 1].reshape(-1, 3 * attn_local))]
        got, _ = lax.optimization_barrier((got, sum_embed[:8]))
        sum_fc2 = r_fc2[:ff_local] + got[0]
        sum_dense = (r_dense[:attn_local] + got[1]).reshape(heads_local, head_dim, -1)
        sum_fc1 = r_fc1[:, :ff_local] + got[2]
        sum_qkv = (r_qkv[:, :, 0] + got[3].reshape(-1, 3, heads_local, head_dim)).transpose(0, 2, 1, 3)

        bqkv_grad = small_sum[5].reshape(3, 2, heads_local, head_dim).transpose(1, 2, 0, 3).reshape(2, -1)
        side = jnp.concatenate([bqkv_grad, small_sum[6].reshape(2, -1)], axis=1)
        side = jnp.where(tp_i == 0, side, side[::-1])
        packed = lax.psum(jnp.concatenate(small_sum[:5] + [side[0], side[1]]), ('tp', 'dp'))
        piece = d_model // n_dp
        common = [lax.dynamic_slice_in_dim(packed, i * d_model + dp_i * piece, piece, 0) for i in range(5)]
        base = 5 * d_model + tp_i * side.shape[1]
        n_b, n_f = 3 * attn_local // n_dp, ff_local // n_dp
        sum_bqkv = lax.dynamic_slice_in_dim(packed, base + dp_i * n_b, n_b, 0)
        sum_bfc1 = lax.dynamic_slice_in_dim(packed, base + 3 * attn_local + dp_i * n_f, n_f, 0)
        return (layer_out, sum_embed, common[0], common[1], common[2], common[3], sum_qkv, sum_bqkv, sum_dense, common[4], sum_fc1, sum_bfc1, sum_fc2, common[4])

    return jax.shard_map(device_step, mesh=mesh, in_specs=arg_specs, out_specs=out_specs, check_vma=False)
```
